8 devices in a mesh: col: 2 (over z, y), row: 4 (over x, core).
Axes of the slice: x: 2, y: 2, z: 1, core: 2. Of those that a mesh axis runs over, the one named last changes fastest.
Arguments:
- trans_mat: bfloat16 [24576, 24576], P('row', 'col')
- x_start: float32 [24576, 512], P(('col', 'row'))
- teleport: float32 [24576, 512], P(('col', 'row'))
- dangling: int32 [24576], P(('col', 'row'))
Outputs:
- output: float32 [24576, 512], P(('col', 'row'))
All inputs are finite; a program needn't handle non-finite values.
Results may differ from the reference program's by a relative error of at most 0.001.
Values are sent between devices in bfloat16 or wider.
A program may use at most 1 GiB of HBM per device.

```python
import jax
import jax.numpy as jnp
from jax import lax

VERTICES = 24576
VECS = 512
DEGREE = 2
SWEEPS = 8
DAMPING = 0.85


def draw_graph(key_dang, key_target, key_edge):
    dangling = (jax.random.randint(key_dang, (VERTICES,), 0, 5) == 0).astype(jnp.int32)
    live_cols = (1 - dangling).astype(jnp.bfloat16)
    target = jax.random.randint(key_target, (VERTICES,), 0, VERTICES)
    row_blocks = 16
    block_rows = VERTICES // row_blocks
    block_keys = jax.random.split(key_edge, row_blocks)
    block_starts = jnp.arange(row_blocks, dtype=jnp.int32) * block_rows

    def edge_block(block_args):
        block_key, block_start = block_args
        draw_vals = jax.random.randint(block_key, (block_rows, VERTICES), 0, VERTICES)
        row_ids = block_start + jnp.arange(block_rows, dtype=jnp.int32)[:, None]
        edge_mask = (draw_vals < DEGREE) | (row_ids == target[None, :])
        return edge_mask.astype(jnp.bfloat16) * live_cols[None, :]

    adjacency = lax.map(edge_block, (block_keys, block_starts)).reshape(VERTICES, VERTICES)
    out_degree = jnp.sum(adjacency, axis=0, dtype=jnp.float32)
    inv_degree = (1.0 / jnp.maximum(out_degree, 1.0)).astype(jnp.bfloat16)
    trans_mat = adjacency * inv_degree[None, :]
    return trans_mat, dangling


def setup_inputs(seed: int = 0) -> dict:
    base_key = jax.random.key(seed)
    k_dang, k_target, k_edge, k_start, k_scale, k_center, k_weight = jax.random.split(base_key, 7)
    trans_mat, dangling = draw_graph(k_dang, k_target, k_edge)
    col_scale = 2.0 ** jax.random.uniform(k_scale, (1, VECS), jnp.float32, -2.0, 2.0)
    x_start = jax.random.uniform(k_start, (VERTICES, VECS), jnp.float32, 0.0, 2.0) * col_scale
    centers = jax.random.randint(k_center, (1, VECS), 0, VERTICES)
    offsets = (jnp.arange(VERTICES, dtype=jnp.int32)[:, None] - centers) % VERTICES
    inside = (offsets < VERTICES // 8).astype(jnp.float32)
    raw_tele = inside * jax.random.uniform(k_weight, (VERTICES, VECS), jnp.float32, 0.5, 2.0)
    teleport = raw_tele * (VERTICES / jnp.sum(raw_tele, axis=0, keepdims=True))
    return {'trans_mat': trans_mat, 'x_start': x_start, 'teleport': teleport, 'dangling': dangling}


def reference(trans_mat, x_start, teleport, dangling):
    dang_col = dangling.astype(jnp.float32)[:, None]

    def one_sweep(x_cur, unused):
        dang_mass = jnp.sum(dang_col * x_cur, axis=0) / VERTICES
        spread = jnp.dot(trans_mat, x_cur.astype(jnp.bfloat16), preferred_element_type=jnp.float32)
        x_next = DAMPING * spread + (DAMPING * dang_mass + (1.0 - DAMPING))[None, :] * teleport
        return x_next, None

    x_final, unused_out = lax.scan(one_sweep, x_start, None, length=SWEEPS)
    return x_final
```

```python
import functools

import jax
import jax.numpy as jnp
from jax import lax
from jax.experimental import pallas as pl
from jax.experimental.pallas import tpu as pltpu
from jax.sharding import PartitionSpec as P

SWEEPS = 8
DAMPING = 0.85
MESH = pl.DeviceIdType.MESH
HALVES = 2
PHASES = SWEEPS * HALVES
GROUPS = 4
CHUNKS = 3 * GROUPS
KSTEPS = 6
FIRST_FINAL = PHASES - HALVES
LIVE_GROUPS = FIRST_FINAL * GROUPS
TOTAL_GROUPS = PHASES * GROUPS


def rcopy(src, dst, send_sem, recv_sem, dev):
    return pltpu.make_async_remote_copy(src_ref=src, dst_ref=dst, send_sem=send_sem, recv_sem=recv_sem,
                                        device_id={"col": dev[0], "row": dev[1]}, device_id_type=MESH)


def kernel(a_ref, x0_ref, v_ref, w_ref, m0_ref, out_ref, vt_ref,
           xs, abuf, acc, part, recv, bst, vbuf, wbuf, mrecv, cvec, fin,
           a_sem, v_sem, w_sem, o_sem,
           fs, fr, bs, br, xsend, xrecv, csend, crecv,
           gx_s, gx_r, gc_s, gc_r, gl_s, gl_r, g_loc, vs, vr,
           ms, mr, fin_r, cred_f, cred_c, cred_x):
    col, row = lax.axis_index("col"), lax.axis_index("row")
    core = lax.rem(row, 2)
    home = col == row // 2
    far = jnp.logical_not(home)
    ydev = (1 - col, row)
    xdev = (col, lax.rem(row + 2, 4))
    cdev = (col, row + 1 - 2 * core)
    me = col * 4 + row
    n_rows, n_cols = a_ref.shape
    verts = n_cols * 2
    rows = n_rows // CHUNKS
    depth = n_cols // KSTEPS
    piece = n_rows // 2
    width = x0_ref.shape[2]
    own_base = core * n_rows

    def every_other(k):
        d = lax.rem(me + k, 8)
        return (d // 4, lax.rem(d, 4))

    barrier = pltpu.get_barrier_semaphore()
    for k in range(1, 8):
        d = every_other(k)
        pl.semaphore_signal(barrier, inc=1, device_id={"col": d[0], "row": d[1]}, device_id_type=MESH)
    pl.semaphore_wait(barrier, 7)

    def a_copy(n, kb):
        return pltpu.make_async_copy(
            a_ref.at[pl.ds(pl.multiple_of(n * rows, rows), rows),
                     pl.ds(pl.multiple_of(kb * depth, depth), depth)],
            abuf.at[kb], a_sem.at[kb])

    for kb in range(KSTEPS):
        a_copy(0, kb).start()

    def x_rows(h, r):
        return xs.at[h, pl.ds(pl.multiple_of(r * piece, piece), piece), :]

    def gather_own(h):
        return pltpu.make_async_copy(x0_ref.at[h], x_rows(h, row), g_loc.at[h])

    def gather_x(h):
        return rcopy(x0_ref.at[h], x_rows(h, row), gx_s.at[h], gx_r.at[h], xdev)

    def gather_c(h):
        return rcopy(x0_ref.at[h], x_rows(h, row), gc_s.at[h], gc_r.at[h], cdev)

    def gather_relay(h):
        r = lax.rem(row + 2, 4)
        return rcopy(x_rows(h, r), x_rows(h, r), gl_s.at[h], gl_r.at[h], cdev)

    keeper = (col, 2 * col + row // 2)
    keeps = jnp.logical_and(home, row == keeper[1])
    side = lax.rem(row, 2)

    def tele_send(h, m):
        src = v_ref.at[pl.ds(m * rows, rows), pl.ds(h * width, width)]
        dst = vt_ref.at[h, pl.ds(pl.multiple_of(side * piece + m * rows, rows), rows), :]
        return rcopy(src, dst, vs.at[h, m], vr.at[h, side * GROUPS + m + 2 * side], keeper)

    def mass_copy(slot, k):
        return rcopy(mrecv.at[slot, me], mrecv.at[slot, me], ms.at[slot], mr.at[slot], every_other(k))

    for h in range(HALVES):
        mrecv[2 + h, me] = m0_ref[h]
        for k in range(1, 8):
            mass_copy(2 + h, k).start()
    gather_x(0).start()
    gather_c(0).start()
    gather_own(0).start()

    @pl.when(jnp.logical_not(keeps))
    def _():
        for m in range(CHUNKS // 2):
            tele_send(0, m).start()

    gather_x(1).start()
    gather_c(1).start()
    gather_own(1).start()

    @pl.when(jnp.logical_not(keeps))
    def _():
        for m in range(CHUNKS // 2):
            tele_send(1, m).start()

    def gather_finish(h):
        gather_x(h).wait_recv()
        gather_relay(h).start()
        gather_own(h).wait()
        gather_c(h).wait_recv()
        gather_relay(h).wait_recv()
        gather_x(h).wait_send()
        gather_c(h).wait_send()
        gather_relay(h).wait_send()

    def own_rows(b, n):
        return xs.at[b, pl.ds(pl.multiple_of(own_base + n * rows, rows), rows), :]

    def partner_rows(b):
        return xs.at[b, pl.ds(pl.multiple_of(n_rows - own_base, n_rows), n_rows), :]

    def place(g, p):
        q = lax.div(g, GROUPS)
        n = lax.rem(g, GROUPS) * 3 + p
        return q, n, lax.rem(q + 2, 3), lax.rem(g, 2)

    def partial_send(g, p):
        slot = lax.rem(g, 2)
        return rcopy(part.at[p, slot], recv.at[p, slot], fs.at[p, slot], fr.at[p, slot], ydev)

    def back_send(g, p):
        q, n, b, slot = place(g, p)
        return rcopy(bst.at[p, slot], own_rows(b, n), bs.at[p, slot], br.at[p, slot], ydev)

    def x_send(g, p):
        q, n, b, slot = place(g, p)
        return rcopy(own_rows(b, n), own_rows(b, n), xsend.at[p], xrecv.at[lax.rem(q, 2), n], xdev)

    def c_send(g, p):
        q, n, b, slot = place(g, p)
        return rcopy(own_rows(b, n), own_rows(b, n), csend.at[p], crecv.at[b], cdev)

    def live(g):
        return jnp.logical_and(g >= 0, g < LIVE_GROUPS)

    def w_copy(n):
        return pltpu.make_async_copy(w_ref.at[pl.ds(pl.multiple_of(n * rows, rows), rows), :], wbuf, w_sem)

    def reduce_chunk(g, p):
        q, n, b, slot = place(g, p)
        x = part[p, slot] + recv[p, slot]
        w = wbuf[...]
        lanes = w.shape[1]
        wx = jnp.concatenate([x[:, k * lanes:(k + 1) * lanes] * w for k in range(width // lanes)], axis=1)
        m = jnp.sum(wx.reshape(rows // 8, 8, width), axis=0)
        ms_slot = lax.rem(q, 4)
        mrecv[ms_slot, me] = mrecv[ms_slot, me] + m
        return x.astype(jnp.bfloat16)

    def final_owner(n):
        return (row // 2, lax.rem(2 * row, 4) + lax.div(n, CHUNKS // 2))

    role = jnp.where(home, 0, 1)

    def final_send(g, p):
        q, n, b, slot = place(g, p)
        m = lax.rem(n, CHUNKS // 2)
        f = q - FIRST_FINAL
        return rcopy(part.at[p, slot], fin.at[f, role, m], fs.at[p, slot], fin_r.at[f, role, m], final_owner(n))

    def final_local(g, p):
        q, n, b, slot = place(g, p)
        o = final_owner(n)
        return jnp.logical_and(o[0] == col, o[1] == row)

    def out_copy(f, m):
        return pltpu.make_async_copy(
            fin.at[f, 0, m],
            out_ref.at[pl.ds(pl.multiple_of(m * rows, rows), rows), pl.ds(pl.multiple_of(f * width, width), width)],
            o_sem)

    src_tile = 2 * col + row // 2

    def final_reduce(f, m):
        tele = pltpu.make_async_copy(
            v_ref.at[pl.ds(pl.multiple_of(m * rows, rows), rows), pl.ds(pl.multiple_of(f * width, width), width)],
            vbuf, v_sem)
        tele.start()
        for r in range(2):
            mine = jnp.logical_and(src_tile == row, home) if r == 0 else jnp.bool_(False)

            @pl.when(jnp.logical_not(mine))
            def _():
                rcopy(fin.at[f, r, m], fin.at[f, r, m], fs.at[0, 0], fin_r.at[f, r, m], cdev).wait_recv()
        tele.wait()
        fin[f, 0, m] = (fin[f, 0, m] + fin[f, 1, m]) + cvec[f] * vbuf[...]
        out_copy(f, m).start()

    def substep(g, p):
        kind = 2 if p < 2 else 1
        q, n, _, slot = place(g, p)
        b = lax.rem(q, 3)
        h = lax.rem(q, 2)
        is_live = g < LIVE_GROUPS

        acc[...] = jnp.zeros_like(acc)
        last = jnp.logical_and(g == TOTAL_GROUPS - 1, p == 2)
        n_next = lax.rem(n + 1, CHUNKS)
        own_tele = jnp.logical_and(row == 2 * col + row // 2,
                                   lax.rem(row, 2) == lax.div(n, CHUNKS // 2))
        take_tele = jnp.logical_and(home, is_live)

        def tele_own():
            return pltpu.make_async_copy(
                v_ref.at[pl.ds(pl.multiple_of(lax.rem(n, CHUNKS // 2) * rows, rows), rows),
                         pl.ds(pl.multiple_of(h * width, width), width)], vbuf, v_sem)

        def tele_got():
            return pltpu.make_async_copy(vt_ref.at[h, pl.ds(pl.multiple_of(n * rows, rows), rows), :], vbuf, v_sem)

        @pl.when(jnp.logical_and(take_tele, own_tele))
        def _():
            tele_own().start()

        @pl.when(jnp.logical_and(take_tele, jnp.logical_not(own_tele)))
        def _():
            @pl.when(q < HALVES)
            def _():
                rcopy(vt_ref.at[h, pl.ds(pl.multiple_of(n * rows, rows), rows), :],
                      vt_ref.at[h, pl.ds(pl.multiple_of(n * rows, rows), rows), :],
                      vs.at[0, 0], vr.at[h, n], cdev).wait_recv()
            tele_got().start()

        def kstep(kb, carry):
            a_copy(n, kb).wait()
            acc[...] += jnp.dot(abuf[kb], xs[b, pl.ds(pl.multiple_of(kb * depth, depth), depth), :],
                                preferred_element_type=jnp.float32)

            @pl.when(jnp.logical_not(last))
            def _():
                a_copy(n_next, kb).start()
            return carry

        lax.fori_loop(0, KSTEPS, kstep, 0)

        if p == 2:
            @pl.when(jnp.logical_and(lax.rem(g, GROUPS) == GROUPS - 1, q < FIRST_FINAL - 1))
            def _():
                pl.semaphore_signal(cred_c, inc=1, device_id={"col": cdev[0], "row": cdev[1]}, device_id_type=MESH)

                @pl.when(far)
                def _():
                    pl.semaphore_signal(cred_x, inc=1, device_id={"col": xdev[0], "row": xdev[1]},
                                        device_id_type=MESH)

        if kind == 2:
            @pl.when(live(g - 4))
            def _():
                @pl.when(far)
                def _():
                    c_send(g - 4, p).wait_send()

            @pl.when(live(g - 3))
            def _():
                @pl.when(far)
                def _():
                    x_send(g - 3, p).wait_recv()
                    c_send(g - 3, p).start()

                @pl.when(home)
                def _():
                    x_send(g - 3, p).wait_send()
                    c_send(g - 3, p).wait_send()

            @pl.when(live(g - 2))
            def _():
                @pl.when(home)
                def _():
                    partial_send(g - 2, p).wait_send()
                    back_send(g - 2, p).wait_recv()
                    x_send(g - 2, p).start()
                    c_send(g - 2, p).start()
        else:
            @pl.when(live(g - 3))
            def _():
                @pl.when(far)
                def _():
                    c_send(g - 3, p).wait_send()

            @pl.when(live(g - 2))
            def _():
                @pl.when(far)
                def _():
                    x_send(g - 2, p).wait_recv()
                    c_send(g - 2, p).start()
                    partial_send(g - 2, p).wait_send()

                @pl.when(home)
                def _():
                    x_send(g - 2, p).wait_send()
                    c_send(g - 2, p).wait_send()

        @pl.when(g - 2 >= LIVE_GROUPS)
        def _():
            @pl.when(jnp.logical_not(final_local(g - 2, p)))
            def _():
                final_send(g - 2, p).wait_send()

        @pl.when(is_live)
        def _():
            @pl.when(home)
            def _():
                @pl.when(own_tele)
                def _():
                    tele_own().wait()

                @pl.when(jnp.logical_not(own_tele))
                def _():
                    tele_got().wait()
                part[p, slot] = DAMPING * acc[...] + cvec[h] * vbuf[...]
                if kind == 2:
                    partial_send(g, p).start()

            @pl.when(far)
            def _():
                part[p, slot] = DAMPING * acc[...]
                if kind == 1:
                    @pl.when(g >= 2)
                    def _():
                        pl.semaphore_wait(cred_f, 1)
                    partial_send(g, p).start()

        @pl.when(jnp.logical_not(is_live))
        def _():
            @pl.when(final_local(g, p))
            def _():
                fin[q - FIRST_FINAL, 0, lax.rem(n, CHUNKS // 2)] = DAMPING * acc[...]

            @pl.when(jnp.logical_not(final_local(g, p)))
            def _():
                part[p, slot] = DAMPING * acc[...]
                final_send(g, p).start()

        @pl.when(live(g - 1))
        def _():
            q1, n1, b1, slot1 = place(g - 1, p)

            @pl.when(far if kind == 2 else home)
            def _():
                w_copy(n1).start()
                partial_send(g - 1, p).wait_recv()
                w_copy(n1).wait()
                if kind == 2:
                    @pl.when(g - 3 >= 0)
                    def _():
                        back_send(g - 3, p).wait_send()
                    bst[p, slot1] = reduce_chunk(g - 1, p)
                    back_send(g - 1, p).start()
                else:
                    xs[b1, pl.ds(pl.multiple_of(own_base + n1 * rows, rows), rows), :] = reduce_chunk(g - 1, p)
                    x_send(g - 1, p).start()
                    c_send(g - 1, p).start()

                    @pl.when(g - 1 < LIVE_GROUPS - 2)
                    def _():
                        pl.semaphore_signal(cred_f, inc=1, device_id={"col": ydev[0], "row": ydev[1]},
                                            device_id_type=MESH)

    def group(g, carry):
        q, gq = lax.div(g, GROUPS), lax.rem(g, GROUPS)

        @pl.when(gq == 0)
        def _():
            @pl.when(q == 0)
            def _():
                gather_finish(0)

            @pl.when(q == 1)
            def _():
                gather_finish(1)

            @pl.when(q >= HALVES)
            def _():
                b = lax.rem(q, 3)
                rcopy(partner_rows(b), partner_rows(b), csend.at[0], crecv.at[b], cdev).wait_recv()

            slot = lax.rem(q + 2, 4)
            others = mrecv.at[slot, pl.ds(0, 7)]
            whole = rcopy(others, others, ms.at[slot], mr.at[slot], cdev)
            whole.wait_recv()
            whole.wait_send()
            mass = jnp.sum(jnp.sum(mrecv[slot], axis=0), axis=0, keepdims=True) / verts
            cvec[lax.rem(q, 2)] = DAMPING * mass + (1.0 - DAMPING)

        @pl.when(gq == 1)
        def _():
            @pl.when(jnp.logical_and(q >= 1, q - 1 < FIRST_FINAL))
            def _():
                slot = lax.rem(q - 1, 4)
                for k in range(1, 8):
                    mass_copy(slot, k).start()

            @pl.when(q < FIRST_FINAL)
            def _():
                mrecv[lax.rem(q, 4), me] = jnp.zeros((8, width), jnp.float32)

                @pl.when(q >= 1)
                def _():
                    pl.semaphore_wait(cred_c, 1)

                    @pl.when(home)
                    def _():
                        pl.semaphore_wait(cred_x, 1)

        for p in range(3):
            substep(g, p)
        return carry

    lax.fori_loop(0, TOTAL_GROUPS, group, 0)

    def finish(f):
        def body(m, carry):
            final_reduce(f, m)
            return carry
        lax.fori_loop(0, CHUNKS // 2, body, 0)

    for f in range(HALVES):
        finish(f)
    for g in (TOTAL_GROUPS - 2, TOTAL_GROUPS - 1):
        for p in range(3):
            @pl.when(jnp.logical_not(final_local(jnp.int32(g), p)))
            def _():
                final_send(jnp.int32(g), p).wait_send()
    for p in range(2):
        for g in (LIVE_GROUPS - 2, LIVE_GROUPS - 1):
            @pl.when(far)
            def _():
                back_send(jnp.int32(g), p).wait_send()

    @pl.when(jnp.logical_not(keeps))
    def _():
        for h in range(HALVES):
            for m in range(CHUNKS // 2):
                tele_send(h, m).wait_send()

    def drain(k, carry):
        out_copy(0, 0).wait()
        return carry
    lax.fori_loop(0, HALVES * (CHUNKS // 2), drain, 0)


def solution(mesh):
    def step(mat, x_piece, v_piece, dang_piece):
        i = lax.axis_index('row')
        j = lax.axis_index('col')
        n_rows, n_cols = mat.shape
        piece, vecs = x_piece.shape
        width = vecs // HALVES
        rows, depth = n_rows // CHUNKS, n_cols // KSTEPS
        lanes = min(128, width)

        dang_f = dang_piece.astype(jnp.float32)
        dang_all = lax.all_gather(dang_f, ('col', 'row'), axis=0, tiled=True)
        tile = lax.dynamic_slice(dang_all, (i * n_rows,), (n_rows,))
        weight = jnp.broadcast_to(tile[:, None], (n_rows, lanes))
        x0 = jnp.stack([x_piece[:, h * width:(h + 1) * width] for h in range(HALVES)]).astype(jnp.bfloat16)
        m0 = jnp.sum((dang_f[:, None] * x_piece).reshape(piece // 8, 8, vecs), axis=0)
        m0 = jnp.stack([m0[:, h * width:(h + 1) * width] for h in range(HALVES)])

        f32, bf16 = jnp.float32, jnp.bfloat16
        dma = pltpu.SemaphoreType.DMA
        hbm = pl.BlockSpec(memory_space=pl.ANY)
        out, _ = pl.pallas_call(
            kernel,
            out_shape=[jax.ShapeDtypeStruct((piece, vecs), f32),
                       jax.ShapeDtypeStruct((HALVES, n_rows, width), f32)],
            in_specs=[hbm, hbm, hbm, hbm, pl.BlockSpec(memory_space=pltpu.VMEM)],
            out_specs=[hbm, hbm],
            scratch_shapes=[
                pltpu.VMEM((3, n_cols, width), bf16),
                pltpu.VMEM((KSTEPS, rows, depth), bf16),
                pltpu.VMEM((rows, width), f32),
                pltpu.VMEM((3, 2, rows, width), f32),
                pltpu.VMEM((3, 2, rows, width), f32),
                pltpu.VMEM((2, 2, rows, width), bf16),
                pltpu.VMEM((rows, width), f32),
                pltpu.VMEM((rows, lanes), f32),
                pltpu.VMEM((4, 8, 8, width), f32),
                pltpu.VMEM((2, 1, width), f32),
                pltpu.VMEM((2, 2, CHUNKS // 2, rows, width), f32),
                dma((KSTEPS,)), dma, dma, dma,
                dma((3, 2)), dma((3, 2)), dma((2, 2)), dma((2, 2)),
                dma((3,)), dma((2, CHUNKS)), dma((3,)), dma((3,)),
                dma((2,)), dma((2,)), dma((2,)), dma((2,)), dma((2,)), dma((2,)), dma((2,)),
                dma((2, CHUNKS // 2)), dma((2, CHUNKS)),
                dma((4,)), dma((4,)), dma((2, 2, CHUNKS // 2)),
                pltpu.SemaphoreType.REGULAR, pltpu.SemaphoreType.REGULAR, pltpu.SemaphoreType.REGULAR,
            ],
            compiler_params=pltpu.CompilerParams(collective_id=0, has_side_effects=True,
                                                 vmem_limit_bytes=62 * 1024 * 1024),
            cost_estimate=pl.CostEstimate(flops=2 * n_rows * n_cols * vecs * SWEEPS,
                                          bytes_accessed=n_rows * n_cols * 2 * PHASES, transcendentals=0),
        )(mat, x0, v_piece, weight, m0)
        return out

    vec = P(('col', 'row'), None)
    return jax.shard_map(step, mesh=mesh, in_specs=(P('row', 'col'), vec, vec, P(('col', 'row'))),
                         out_specs=vec, check_vma=False)
```

```python
import jax
import jax.numpy as jnp
from jax import lax
from jax.experimental import pallas as pl
from jax.experimental.pallas import tpu as pltpu
from jax.sharding import PartitionSpec as P

SWEEPS = 8
DAMPING = 0.85
MESH = pl.DeviceIdType.MESH
HALVES = 2
PHASES = SWEEPS * HALVES
GROUPS = 3
CHUNKS = 4 * GROUPS
PIECE_CHUNKS = CHUNKS // 2
KSTEPS = 6
UNITS = (7, 9, 7, 9)
FIRST_FINAL = PHASES - HALVES
LIVE_GROUPS = FIRST_FINAL * GROUPS
TOTAL_GROUPS = PHASES * GROUPS


def rcopy(src, dst, send_sem, recv_sem, dev):
    return pltpu.make_async_remote_copy(src_ref=src, dst_ref=dst, send_sem=send_sem, recv_sem=recv_sem,
                                        device_id={"col": dev[0], "row": dev[1]}, device_id_type=MESH)


def signal(sem, dev):
    pl.semaphore_signal(sem, inc=1, device_id={"col": dev[0], "row": dev[1]}, device_id_type=MESH)


def kernel(a_ref, x0_ref, v_ref, w_ref, m0_ref, out_ref, vt_ref,
           xs, abuf, acc, part0, part1, part2, part3, recv0, recv1, recv3, side_in, cross_in, bst, round_in,
           vbuf, wbuf, mrecv, cvec, fin,
           a_sem, v_sem, w_sem, o_sem,
           fs, fr, side_r, cross_s, cross_r, bs, round_r, round_s, yrecv, xsend, xrecv, csend, crecv,
           gx_s, gx_r, gc_s, gc_r, gl_s, gl_r, g_loc, vs, vr,
           ms, mr, fin_r, cred_f, cred_side, cred_cross, cred_round, cred_c, cred_x, cred_y):
    col, row = lax.axis_index("col"), lax.axis_index("row")
    core = lax.rem(row, 2)
    home = col == row // 2
    far = jnp.logical_not(home)
    ydev = (1 - col, row)
    xdev = (col, lax.rem(row + 2, 4))
    cdev = (col, row + 1 - 2 * core)
    me = col * 4 + row
    n_rows, n_cols = a_ref.shape
    verts = n_cols * 2
    unit = n_rows // 96
    size = tuple(u * unit for u in UNITS)
    start = (0, size[0], size[0] + size[1], size[0] + size[1] + size[2])
    span = sum(size)
    depth = n_cols // KSTEPS
    piece = n_rows // 2
    width = x0_ref.shape[2]
    own_base = core * n_rows
    parts = (part0, part1, part2, part3)
    recvs = (recv0, recv1, None, recv3)

    def every_other(k):
        d = lax.rem(me + k, 8)
        return (d // 4, lax.rem(d, 4))

    barrier = pltpu.get_barrier_semaphore()
    for k in range(1, 8):
        signal(barrier, every_other(k))
    pl.semaphore_wait(barrier, 7)

    def tile_rows(gq, p):
        return pl.ds(pl.multiple_of(gq * span + start[p], unit), size[p])

    def half_cols(h):
        return pl.ds(pl.multiple_of(h * width, width), width)

    def a_copy(gq, p, kb):
        return pltpu.make_async_copy(
            a_ref.at[tile_rows(gq, p), pl.ds(pl.multiple_of(kb * depth, depth), depth)],
            abuf.at[kb, pl.ds(0, size[p])], a_sem.at[kb])

    for kb in range(KSTEPS):
        a_copy(0, 0, kb).start()

    def x_rows(h, r):
        return xs.at[h, pl.ds(pl.multiple_of(r * piece, piece), piece), :]

    def gather_own(h):
        return pltpu.make_async_copy(x0_ref.at[h], x_rows(h, row), g_loc.at[h])

    def gather_x(h):
        return rcopy(x0_ref.at[h], x_rows(h, row), gx_s.at[h], gx_r.at[h], xdev)

    def gather_c(h):
        return rcopy(x0_ref.at[h], x_rows(h, row), gc_s.at[h], gc_r.at[h], cdev)

    def gather_relay(h):
        r = lax.rem(row + 2, 4)
        return rcopy(x_rows(h, r), x_rows(h, r), gl_s.at[h], gl_r.at[h], cdev)

    keeper = (col, 2 * col + row // 2)
    keeps = jnp.logical_and(home, row == keeper[1])

    def piece_start(m):
        return (m // 2) * (size[0] + size[1]) + (m % 2) * size[0]

    def tele_send(h, m):
        rows = size[m % 2]
        src = v_ref.at[pl.ds(piece_start(m), rows), pl.ds(h * width, width)]
        dst = vt_ref.at[h, pl.ds(pl.multiple_of(core * piece + piece_start(m), unit), rows), :]
        return rcopy(src, dst, vs.at[h, m], vr.at[h, core * PIECE_CHUNKS + m], keeper)

    def mass_copy(slot, k):
        return rcopy(mrecv.at[slot, me], mrecv.at[slot, me], ms.at[slot], mr.at[slot], every_other(k))

    for h in range(HALVES):
        mrecv[2 + h, me] = m0_ref[h]
        for k in range(1, 8):
            mass_copy(2 + h, k).start()

    for h in range(HALVES):
        gather_x(h).start()
        gather_c(h).start()
        gather_own(h).start()

        @pl.when(jnp.logical_not(keeps))
        def _():
            for m in range(PIECE_CHUNKS):
                tele_send(h, m).start()

    def gather_finish(h):
        gather_x(h).wait_recv()
        gather_relay(h).start()
        gather_own(h).wait()
        gather_c(h).wait_recv()
        gather_relay(h).wait_recv()
        gather_x(h).wait_send()
        gather_c(h).wait_send()
        gather_relay(h).wait_send()

    def live(g):
        return jnp.logical_and(g >= 0, g < LIVE_GROUPS)

    def own_rows(g, p):
        b = lax.rem(lax.div(g, GROUPS) + 2, 3)
        gq = lax.rem(g, GROUPS)
        return xs.at[b, pl.ds(pl.multiple_of(own_base + gq * span + start[p], unit), size[p]), :]

    def chunk_of(g, p):
        return lax.rem(g, GROUPS) * 4 + p

    def parity(g):
        return lax.rem(lax.div(g, GROUPS), 2)

    def f_send(g, p):
        slot = lax.rem(g, 2)
        return rcopy(parts[p].at[slot], recvs[p].at[slot], fs.at[p, slot], fr.at[p, slot], ydev)

    def side_send(g):
        slot, in_slot = lax.rem(g, 2), lax.rem(g, 3)
        return rcopy(part2.at[slot], side_in.at[in_slot], fs.at[2, slot], side_r.at[in_slot], xdev)

    def cross_send(g):
        slot, in_slot = lax.rem(g, 2), lax.rem(g, 3)
        return rcopy(side_in.at[in_slot], cross_in.at[slot], cross_s, cross_r.at[slot], ydev)

    def round_send(g):
        slot, in_slot = lax.rem(g, 2), lax.rem(g, 4)
        return rcopy(bst.at[slot], round_in.at[in_slot], bs.at[slot], round_r.at[in_slot], xdev)

    def round_pass(g):
        in_slot = lax.rem(g, 4)
        return rcopy(round_in.at[in_slot], own_rows(g, 0), round_s, yrecv.at[parity(g), lax.rem(g, GROUPS)], ydev)

    def x_send(g, p):
        return rcopy(own_rows(g, p), own_rows(g, p), xsend.at[p], xrecv.at[parity(g), chunk_of(g, p)], xdev)

    def c_send(g, p):
        b = lax.rem(lax.div(g, GROUPS) + 2, 3)
        return rcopy(own_rows(g, p), own_rows(g, p), csend.at[p], crecv.at[b], cdev)

    def w_copy(which, g, p):
        return pltpu.make_async_copy(w_ref.at[which, tile_rows(lax.rem(g, GROUPS), p), :],
                                     wbuf.at[pl.ds(0, size[p])], w_sem)

    def new_rows(g, p, one, two):
        x = one + two
        w = wbuf[0:size[p]]
        lanes = w.shape[1]
        wx = jnp.concatenate([x[:, k * lanes:(k + 1) * lanes] * w for k in range(width // lanes)], axis=1)
        slot = lax.rem(lax.div(g, GROUPS), 4)
        mrecv[slot, me] = mrecv[slot, me] + jnp.sum(wx.reshape(size[p] // 8, 8, width), axis=0)
        return x.astype(jnp.bfloat16)

    def put_rows(g, p, value):
        b = lax.rem(lax.div(g, GROUPS) + 2, 3)
        gq = lax.rem(g, GROUPS)
        xs[b, pl.ds(pl.multiple_of(own_base + gq * span + start[p], unit), size[p]), :] = value

    def share(g, p):
        x_send(g, p).start()
        c_send(g, p).start()

    def sent(g, p, role, both):
        @pl.when(jnp.logical_and(live(g), role))
        def _():
            if both:
                x_send(g, p).wait_send()
            c_send(g, p).wait_send()

    def take_side(g, p, role):
        sent(g - 1, p, role, False)

        @pl.when(jnp.logical_and(live(g), role))
        def _():
            x_send(g, p).wait_recv()
            c_send(g, p).start()

    def credit(sem, dev, g, depth_):
        @pl.when(g < LIVE_GROUPS - depth_)
        def _():
            signal(sem, dev)

    def need(sem, g, depth_):
        @pl.when(g >= depth_)
        def _():
            pl.semaphore_wait(sem, 1)

    def home_reduce(g, p):
        sent(g - 1, p, home, True)

        @pl.when(jnp.logical_and(live(g), home))
        def _():
            slot = lax.rem(g, 2)
            f_send(g, p).wait_recv()
            w_copy(0, g, p).wait()
            put_rows(g, p, new_rows(g, p, parts[p][slot], recvs[p][slot]))
            share(g, p)
            credit(cred_f.at[p], ydev, g, 2)

    def far_reduce(g):
        @pl.when(jnp.logical_and(live(g), far))
        def _():
            slot = lax.rem(g, 2)
            f_send(g, 0).wait_recv()
            w_copy(0, g, 0).wait()

            @pl.when(g >= 2)
            def _():
                round_send(g - 2).wait_send()
            bst[slot] = new_rows(g, 0, part0[slot], recv0[slot])
            need(cred_round, g, 4)
            round_send(g).start()
            credit(cred_f.at[0], ydev, g, 2)

    def round_relay(g):
        @pl.when(jnp.logical_and(live(g - 1), home))
        def _():
            round_pass(g - 1).wait_send()
            credit(cred_round, xdev, g - 1, 4)

        @pl.when(jnp.logical_and(live(g), home))
        def _():
            round_send(g).wait_recv()
            round_pass(g).start()

    def round_take(g):
        sent(g - 1, 0, far, True)

        @pl.when(jnp.logical_and(live(g), far))
        def _():
            round_pass(g).wait_recv()
            share(g, 0)

    def cross_relay(g):
        @pl.when(jnp.logical_and(live(g - 1), home))
        def _():
            cross_send(g - 1).wait_send()
            credit(cred_side, xdev, g - 1, 3)

        @pl.when(jnp.logical_and(live(g), home))
        def _():
            side_send(g).wait_recv()
            need(cred_cross, g, 2)
            cross_send(g).start()

    def cross_reduce(g):
        sent(g - 1, 2, far, True)

        @pl.when(jnp.logical_and(live(g), far))
        def _():
            side_send(g).wait_recv()
            cross_send(g).wait_recv()
            w_copy(1, g, 2).wait()
            put_rows(g, 2, new_rows(g, 2, side_in[lax.rem(g, 3)], cross_in[lax.rem(g, 2)]))
            share(g, 2)
            credit(cred_side, xdev, g, 3)
            credit(cred_cross, ydev, g, 2)

    role = jnp.where(home, 0, 1)

    def final_place(g, p):
        n = chunk_of(g, p)
        side = lax.div(n, PIECE_CHUNKS)
        f = lax.div(g, GROUPS) - FIRST_FINAL
        at = lax.rem(g, GROUPS) * span + start[p] - side * piece
        return f, lax.rem(n, PIECE_CHUNKS), pl.ds(pl.multiple_of(at, unit), size[p]), (row // 2, lax.rem(2 * row, 4) + side)

    def final_send(g, p):
        f, m, rows, owner = final_place(g, p)
        slot = lax.rem(g, 2)
        return rcopy(parts[p].at[slot], fin.at[f, role, rows], fs.at[p, slot], fin_r.at[f, role, m], owner)

    def final_local(g, p):
        owner = final_place(g, p)[3]
        return jnp.logical_and(owner[0] == col, owner[1] == row)

    def fin_rows(j, k):
        return pl.ds(pl.multiple_of(j * (size[0] + size[1]) + k * size[0], unit), size[k])

    def out_copy(f, j, k):
        return pltpu.make_async_copy(fin.at[f, 0, fin_rows(j, k)],
                                     out_ref.at[fin_rows(j, k), half_cols(f)], o_sem)

    own_tile = 2 * col + row // 2 == row

    def final_reduce(f, j, k):
        rows = fin_rows(j, k)
        tele = pltpu.make_async_copy(v_ref.at[rows, half_cols(f)], vbuf.at[pl.ds(0, size[k])], v_sem)
        tele.start()
        for r in range(2):
            skip = jnp.logical_and(own_tile, home) if r == 0 else jnp.bool_(False)

            @pl.when(jnp.logical_not(skip))
            def _():
                rcopy(fin.at[f, r, rows], fin.at[f, r, rows], fs.at[0, 0], fin_r.at[f, r, 2 * j + k], cdev).wait_recv()
        tele.wait()
        fin[f, 0, rows] = (fin[f, 0, rows] + fin[f, 1, rows]) + cvec[f] * vbuf[0:size[k]]
        out_copy(f, j, k).start()

    def substep(g, p):
        q, gq = lax.div(g, GROUPS), lax.rem(g, GROUPS)
        n = gq * 4 + p
        b, h, slot = lax.rem(q, 3), lax.rem(q, 2), lax.rem(g, 2)
        rows = size[p]
        is_live = g < LIVE_GROUPS
        side = lax.div(n, PIECE_CHUNKS)
        own_tele = jnp.logical_and(own_tile, core == side)
        take_tele = jnp.logical_and(home, is_live)

        def tele_own():
            at = gq * span + start[p] - side * piece
            return pltpu.make_async_copy(v_ref.at[pl.ds(pl.multiple_of(at, unit), rows), half_cols(h)],
                                         vbuf.at[pl.ds(0, rows)], v_sem)

        def tele_got():
            return pltpu.make_async_copy(vt_ref.at[h, tile_rows(gq, p), :], vbuf.at[pl.ds(0, rows)], v_sem)

        @pl.when(jnp.logical_and(take_tele, own_tele))
        def _():
            tele_own().start()

        @pl.when(jnp.logical_and(take_tele, jnp.logical_not(own_tele)))
        def _():
            @pl.when(q < HALVES)
            def _():
                got = vt_ref.at[h, tile_rows(gq, p), :]
                rcopy(got, got, vs.at[0, 0], vr.at[h, n], cdev).wait_recv()
            tele_got().start()

        if p in (1, 3):
            @pl.when(jnp.logical_and(live(g - 1), home))
            def _():
                w_copy(0, g - 1, p).start()
        if p == 0:
            @pl.when(jnp.logical_and(live(g - 1), far))
            def _():
                w_copy(0, g - 1, 0).start()
        if p == 1:
            @pl.when(jnp.logical_and(live(g - 2), far))
            def _():
                w_copy(1, g - 2, 2).start()

        acc[0:rows] = jnp.zeros((rows, width), jnp.float32)
        nxt_p = (p + 1) % 4
        nxt_gq = lax.rem(gq + 1, GROUPS) if p == 3 else gq
        more = g < TOTAL_GROUPS - 1 if p == 3 else jnp.bool_(True)

        def kstep(kb, carry):
            a_copy(gq, p, kb).wait()
            acc[0:rows] += jnp.dot(abuf[kb, 0:rows], xs[b, pl.ds(pl.multiple_of(kb * depth, depth), depth), :],
                                   preferred_element_type=jnp.float32)

            @pl.when(more)
            def _():
                a_copy(nxt_gq, nxt_p, kb).start()
            return carry

        lax.fori_loop(0, KSTEPS, kstep, 0)

        if p == 3:
            @pl.when(jnp.logical_and(gq == GROUPS - 1, q < FIRST_FINAL - 1))
            def _():
                signal(cred_c, cdev)

                @pl.when(far)
                def _():
                    signal(cred_x, xdev)
                    signal(cred_y, ydev)

        sender = {0: home, 1: far, 2: jnp.bool_(True), 3: far}[p]

        @pl.when(jnp.logical_and(live(g - 2), sender))
        def _():
            (side_send(g - 2) if p == 2 else f_send(g - 2, p)).wait_send()

        @pl.when(g - 2 >= LIVE_GROUPS)
        def _():
            @pl.when(jnp.logical_not(final_local(g - 2, p)))
            def _():
                final_send(g - 2, p).wait_send()

        @pl.when(is_live)
        def _():
            @pl.when(home)
            def _():
                @pl.when(own_tele)
                def _():
                    tele_own().wait()

                @pl.when(jnp.logical_not(own_tele))
                def _():
                    tele_got().wait()
                parts[p][slot] = DAMPING * acc[0:rows] + cvec[h] * vbuf[0:rows]

            @pl.when(far)
            def _():
                parts[p][slot] = DAMPING * acc[0:rows]

            if p == 2:
                need(cred_side, g, 3)
                side_send(g).start()
            else:
                @pl.when(sender)
                def _():
                    need(cred_f.at[p], g, 2)
                    f_send(g, p).start()

        @pl.when(jnp.logical_not(is_live))
        def _():
            f, m, at, owner = final_place(g, p)

            @pl.when(final_local(g, p))
            def _():
                fin[f, 0, at] = DAMPING * acc[0:rows]

            @pl.when(jnp.logical_not(final_local(g, p)))
            def _():
                parts[p][slot] = DAMPING * acc[0:rows]
                final_send(g, p).start()

        if p == 0:
            take_side(g - 3, 2, home)
            take_side(g - 2, 1, far)
            far_reduce(g - 1)
        if p == 1:
            take_side(g - 3, 0, home)
            cross_reduce(g - 2)
            home_reduce(g - 1, 1)
        if p == 2:
            round_take(g - 2)
            take_side(g - 2, 3, far)
            cross_relay(g - 1)
        if p == 3:
            round_relay(g - 1)
            home_reduce(g - 1, 3)

    def group(g, carry):
        q, gq = lax.div(g, GROUPS), lax.rem(g, GROUPS)

        @pl.when(gq == 0)
        def _():
            @pl.when(q == 0)
            def _():
                gather_finish(0)

            @pl.when(q == 1)
            def _():
                gather_finish(1)

            @pl.when(q >= HALVES)
            def _():
                other = xs.at[lax.rem(q, 3), pl.ds(pl.multiple_of(n_rows - own_base, n_rows), n_rows), :]
                rcopy(other, other, csend.at[0], crecv.at[lax.rem(q, 3)], cdev).wait_recv()

            slot = lax.rem(q + 2, 4)
            others = mrecv.at[slot, pl.ds(0, 7)]
            whole = rcopy(others, others, ms.at[slot], mr.at[slot], cdev)
            whole.wait_recv()
            whole.wait_send()
            mass = jnp.sum(jnp.sum(mrecv[slot], axis=0), axis=0, keepdims=True) / verts
            cvec[lax.rem(q, 2)] = DAMPING * mass + (1.0 - DAMPING)

            @pl.when(q < FIRST_FINAL)
            def _():
                mrecv[lax.rem(q, 4), me] = jnp.zeros((8, width), jnp.float32)

        @pl.when(jnp.logical_and(gq == 1, jnp.logical_and(q >= 1, q < FIRST_FINAL)))
        def _():
            pl.semaphore_wait(cred_c, 1)

            @pl.when(home)
            def _():
                pl.semaphore_wait(cred_x, 1)
                pl.semaphore_wait(cred_y, 1)

        @pl.when(jnp.logical_and(gq == 2, jnp.logical_and(q >= 1, q - 1 < FIRST_FINAL)))
        def _():
            for k in range(1, 8):
                mass_copy(lax.rem(q - 1, 4), k).start()

        for p in range(4):
            substep(g, p)
        return carry

    lax.fori_loop(0, TOTAL_GROUPS, group, 0)

    for f in range(HALVES):
        def body(j, carry):
            final_reduce(f, j, 0)
            final_reduce(f, j, 1)
            return carry
        lax.fori_loop(0, PIECE_CHUNKS // 2, body, 0)

    for g in (TOTAL_GROUPS - 2, TOTAL_GROUPS - 1):
        for p in range(4):
            @pl.when(jnp.logical_not(final_local(jnp.int32(g), p)))
            def _():
                final_send(jnp.int32(g), p).wait_send()

    @pl.when(far)
    def _():
        for g in (LIVE_GROUPS - 2, LIVE_GROUPS - 1):
            round_send(jnp.int32(g)).wait_send()

    @pl.when(jnp.logical_not(keeps))
    def _():
        for h in range(HALVES):
            for m in range(PIECE_CHUNKS):
                tele_send(h, m).wait_send()

    def drain(j, carry):
        out_copy(0, 0, 0).wait()
        out_copy(0, 0, 1).wait()
        return carry
    lax.fori_loop(0, HALVES * PIECE_CHUNKS // 2, drain, 0)


def solution(mesh):
    def step(mat, x_piece, v_piece, dang_piece):
        i = lax.axis_index('row')
        n_rows, n_cols = mat.shape
        piece, vecs = x_piece.shape
        width = vecs // HALVES
        unit, depth = n_rows // 96, n_cols // KSTEPS
        small, large = UNITS[0] * unit, UNITS[1] * unit
        lanes = min(128, width)

        dang_f = dang_piece.astype(jnp.float32)
        dang_all = lax.all_gather(dang_f, ('col', 'row'), axis=0, tiled=True)
        tiles = jnp.stack([lax.dynamic_slice(dang_all, (i * n_rows,), (n_rows,)),
                           lax.dynamic_slice(dang_all, (lax.rem(i + 2, 4) * n_rows,), (n_rows,))])
        weight = jnp.broadcast_to(tiles[:, :, None], (2, n_rows, lanes))
        x0 = jnp.stack([x_piece[:, h * width:(h + 1) * width] for h in range(HALVES)]).astype(jnp.bfloat16)
        m0 = jnp.sum((dang_f[:, None] * x_piece).reshape(piece // 8, 8, vecs), axis=0)
        m0 = jnp.stack([m0[:, h * width:(h + 1) * width] for h in range(HALVES)])

        f32, bf16 = jnp.float32, jnp.bfloat16
        dma, regular = pltpu.SemaphoreType.DMA, pltpu.SemaphoreType.REGULAR
        hbm = pl.BlockSpec(memory_space=pl.ANY)
        out, _ = pl.pallas_call(
            kernel,
            out_shape=[jax.ShapeDtypeStruct((piece, vecs), f32),
                       jax.ShapeDtypeStruct((HALVES, n_rows, width), f32)],
            in_specs=[hbm, hbm, hbm, hbm, pl.BlockSpec(memory_space=pltpu.VMEM)],
            out_specs=[hbm, hbm],
            scratch_shapes=[
                pltpu.VMEM((3, n_cols, width), bf16),
                pltpu.VMEM((KSTEPS, large, depth), bf16),
                pltpu.VMEM((large, width), f32),
                pltpu.VMEM((2, small, width), f32),
                pltpu.VMEM((2, large, width), f32),
                pltpu.VMEM((2, small, width), f32),
                pltpu.VMEM((2, large, width), f32),
                pltpu.VMEM((2, small, width), f32),
                pltpu.VMEM((2, large, width), f32),
                pltpu.VMEM((2, large, width), f32),
                pltpu.VMEM((3, small, width), f32),
                pltpu.VMEM((2, small, width), f32),
                pltpu.VMEM((2, small, width), bf16),
                pltpu.VMEM((4, small, width), bf16),
                pltpu.VMEM((large, width), f32),
                pltpu.VMEM((large, lanes), f32),
                pltpu.VMEM((4, 8, 8, width), f32),
                pltpu.VMEM((2, 1, width), f32),
                pltpu.VMEM((2, 2, piece, width), f32),
                dma((KSTEPS,)), dma, dma, dma,
                dma((4, 2)), dma((4, 2)),
                dma((3,)), dma, dma((2,)),
                dma((2,)), dma((4,)), dma, dma((2, GROUPS)),
                dma((4,)), dma((2, CHUNKS)), dma((4,)), dma((3,)),
                dma((2,)), dma((2,)), dma((2,)), dma((2,)), dma((2,)), dma((2,)), dma((2,)),
                dma((2, PIECE_CHUNKS)), dma((2, CHUNKS)),
                dma((4,)), dma((4,)), dma((2, 2, PIECE_CHUNKS)),
                regular((4,)), regular, regular, regular, regular, regular, regular,
            ],
            compiler_params=pltpu.CompilerParams(collective_id=0, has_side_effects=True,
                                                 vmem_limit_bytes=62 * 1024 * 1024),
            cost_estimate=pl.CostEstimate(flops=2 * n_rows * n_cols * vecs * SWEEPS,
                                          bytes_accessed=n_rows * n_cols * 2 * PHASES, transcendentals=0),
        )(mat, x0, v_piece, weight, m0)
        return out

    vec = P(('col', 'row'), None)
    return jax.shard_map(step, mesh=mesh, in_specs=(P('row', 'col'), vec, vec, P(('col', 'row'))),
                         out_specs=vec, check_vma=False)
```

```python
import jax
import jax.numpy as jnp
from jax import lax
from jax.experimental import pallas as pl
from jax.experimental.pallas import tpu as pltpu
from jax.sharding import PartitionSpec as P

SWEEPS = 8
DAMPING = 0.85
MESH = pl.DeviceIdType.MESH
HALVES = 2
PHASES = SWEEPS * HALVES
GROUPS = 3
CHUNKS = 4 * GROUPS
PIECE_CHUNKS = CHUNKS // 2
UNITS = (7, 9, 7, 9)
FIRST_FINAL = PHASES - HALVES
LIVE_GROUPS = FIRST_FINAL * GROUPS
TOTAL_GROUPS = PHASES * GROUPS


def rcopy(src, dst, send_sem, recv_sem, dev):
    return pltpu.make_async_remote_copy(src_ref=src, dst_ref=dst, send_sem=send_sem, recv_sem=recv_sem,
                                        device_id={"col": dev[0], "row": dev[1]}, device_id_type=MESH)


def signal(sem, dev):
    pl.semaphore_signal(sem, inc=1, device_id={"col": dev[0], "row": dev[1]}, device_id_type=MESH)


def kernel(a_ref, x0_ref, v_ref, w_ref, m0_ref, fin_ref, vt_ref, cvec,
           xs, abuf, acc, part0, part1, part2, part3, recv0, recv1, recv3, side_in, cross_in, bst, round_in,
           vbuf, wbuf, mrecv,
           a_sem, v_sem, w_sem,
           fs, fr, side_r, cross_s, cross_r, bs, round_r, round_s, yrecv, xsend, xrecv, csend, crecv,
           gx_s, gx_r, gc_s, gc_r, gl_s, gl_r, g_loc, vs, vr,
           ms, mr, fin_r, cred_f, cred_side, cred_cross, cred_round, cred_c, cred_x, cred_y):
    col, row = lax.axis_index("col"), lax.axis_index("row")
    core = lax.rem(row, 2)
    home = col == row // 2
    far = jnp.logical_not(home)
    ydev = (1 - col, row)
    xdev = (col, lax.rem(row + 2, 4))
    cdev = (col, row + 1 - 2 * core)
    me = col * 4 + row
    n_rows, n_cols = a_ref.shape
    verts = n_cols * 2
    unit = n_rows // 96
    size = tuple(u * unit for u in UNITS)
    start = (0, size[0], size[0] + size[1], size[0] + size[1] + size[2])
    span = sum(size)
    piece = n_rows // 2
    width = x0_ref.shape[2]
    own_base = core * n_rows
    parts = (part0, part1, part2, part3)
    recvs = (recv0, recv1, None, recv3)

    def every_other(k):
        d = lax.rem(me + k, 8)
        return (d // 4, lax.rem(d, 4))

    def tile_rows(gq, p):
        return pl.ds(pl.multiple_of(gq * span + start[p], unit), size[p])

    def half_cols(h):
        return pl.ds(pl.multiple_of(h * width, width), width)

    def a_copy(gq, p):
        return pltpu.make_async_copy(a_ref.at[tile_rows(gq, p), :], abuf.at[p % 2, pl.ds(0, size[p])], a_sem.at[p % 2])

    for p in range(2):
        a_copy(0, p).start()

    barrier = pltpu.get_barrier_semaphore()
    for k in range(1, 8):
        signal(barrier, every_other(k))
    pl.semaphore_wait(barrier, 7)

    def x_rows(h, r):
        return xs.at[h, pl.ds(pl.multiple_of(r * piece, piece), piece), :]

    def gather_own(h):
        return pltpu.make_async_copy(x0_ref.at[h], x_rows(h, row), g_loc.at[h])

    def gather_x(h):
        return rcopy(x0_ref.at[h], x_rows(h, row), gx_s.at[h], gx_r.at[h], xdev)

    def gather_c(h):
        return rcopy(x0_ref.at[h], x_rows(h, row), gc_s.at[h], gc_r.at[h], cdev)

    def gather_relay(h):
        r = lax.rem(row + 2, 4)
        return rcopy(x_rows(h, r), x_rows(h, r), gl_s.at[h], gl_r.at[h], cdev)

    keeper = (col, 2 * col + row // 2)
    keeps = jnp.logical_and(home, row == keeper[1])

    def piece_start(m):
        return (m // 2) * (size[0] + size[1]) + (m % 2) * size[0]

    def tele_send(h, m):
        rows = size[m % 2]
        src = v_ref.at[pl.ds(piece_start(m), rows), pl.ds(h * width, width)]
        dst = vt_ref.at[h, pl.ds(pl.multiple_of(core * piece + piece_start(m), unit), rows), :]
        return rcopy(src, dst, vs.at[h, m], vr.at[h, core * PIECE_CHUNKS + m], keeper)

    def mass_copy(slot, k):
        return rcopy(mrecv.at[slot, me], mrecv.at[slot, me], ms.at[slot], mr.at[slot], every_other(k))

    for h in range(HALVES):
        mrecv[2 + h, me] = m0_ref[h]
        for k in range(1, 8):
            mass_copy(2 + h, k).start()

    for h in range(HALVES):
        gather_x(h).start()
        gather_c(h).start()
        gather_own(h).start()

        @pl.when(jnp.logical_not(keeps))
        def _():
            for m in range(PIECE_CHUNKS):
                tele_send(h, m).start()

    def gather_finish(h):
        gather_x(h).wait_recv()
        gather_relay(h).start()
        gather_own(h).wait()
        gather_c(h).wait_recv()
        gather_relay(h).wait_recv()
        gather_x(h).wait_send()
        gather_c(h).wait_send()
        gather_relay(h).wait_send()

    def live(g):
        return jnp.logical_and(g >= 0, g < LIVE_GROUPS)

    def own_rows(g, p):
        b = lax.rem(lax.div(g, GROUPS) + 2, 3)
        gq = lax.rem(g, GROUPS)
        return xs.at[b, pl.ds(pl.multiple_of(own_base + gq * span + start[p], unit), size[p]), :]

    def chunk_of(g, p):
        return lax.rem(g, GROUPS) * 4 + p

    def parity(g):
        return lax.rem(lax.div(g, GROUPS), 2)

    def f_send(g, p):
        slot = lax.rem(g, 2)
        return rcopy(parts[p].at[slot], recvs[p].at[slot], fs.at[p, slot], fr.at[p, slot], ydev)

    def side_send(g):
        slot, in_slot = lax.rem(g, 2), lax.rem(g, 3)
        return rcopy(part2.at[slot], side_in.at[in_slot], fs.at[2, slot], side_r.at[in_slot], xdev)

    def cross_send(g):
        slot, in_slot = lax.rem(g, 2), lax.rem(g, 3)
        return rcopy(side_in.at[in_slot], cross_in.at[slot], cross_s, cross_r.at[slot], ydev)

    def round_send(g):
        slot, in_slot = lax.rem(g, 2), lax.rem(g, 4)
        return rcopy(bst.at[slot], round_in.at[in_slot], bs.at[slot], round_r.at[in_slot], xdev)

    def round_pass(g):
        in_slot = lax.rem(g, 4)
        return rcopy(round_in.at[in_slot], own_rows(g, 0), round_s, yrecv.at[parity(g), lax.rem(g, GROUPS)], ydev)

    def x_send(g, p):
        return rcopy(own_rows(g, p), own_rows(g, p), xsend.at[p], xrecv.at[parity(g), chunk_of(g, p)], xdev)

    def c_send(g, p):
        b = lax.rem(lax.div(g, GROUPS) + 2, 3)
        return rcopy(own_rows(g, p), own_rows(g, p), csend.at[p], crecv.at[b], cdev)

    def w_copy(which, g, p):
        return pltpu.make_async_copy(w_ref.at[which, tile_rows(lax.rem(g, GROUPS), p), :],
                                     wbuf.at[pl.ds(0, size[p])], w_sem)

    def new_rows(g, p, one, two):
        x = one + two
        w = wbuf[0:size[p]]
        lanes = w.shape[1]
        wx = jnp.concatenate([x[:, k * lanes:(k + 1) * lanes] * w for k in range(width // lanes)], axis=1)
        slot = lax.rem(lax.div(g, GROUPS), 4)
        mrecv[slot, me] = mrecv[slot, me] + jnp.sum(wx.reshape(size[p] // 8, 8, width), axis=0)
        return x.astype(jnp.bfloat16)

    def put_rows(g, p, value):
        b = lax.rem(lax.div(g, GROUPS) + 2, 3)
        gq = lax.rem(g, GROUPS)
        xs[b, pl.ds(pl.multiple_of(own_base + gq * span + start[p], unit), size[p]), :] = value

    def share(g, p):
        x_send(g, p).start()
        c_send(g, p).start()

    def sent(g, p, role, both):
        @pl.when(jnp.logical_and(live(g), role))
        def _():
            if both:
                x_send(g, p).wait_send()
            c_send(g, p).wait_send()

    def take_side(g, p, role):
        sent(g - 1, p, role, False)

        @pl.when(jnp.logical_and(live(g), role))
        def _():
            x_send(g, p).wait_recv()
            c_send(g, p).start()

    def credit(sem, dev, g, depth_):
        @pl.when(g < LIVE_GROUPS - depth_)
        def _():
            signal(sem, dev)

    def need(sem, g, depth_):
        @pl.when(g >= depth_)
        def _():
            pl.semaphore_wait(sem, 1)

    def home_reduce(g, p):
        sent(g - 1, p, home, True)

        @pl.when(jnp.logical_and(live(g), home))
        def _():
            slot = lax.rem(g, 2)
            f_send(g, p).wait_recv()
            w_copy(0, g, p).wait()
            put_rows(g, p, new_rows(g, p, parts[p][slot], recvs[p][slot]))
            share(g, p)
            credit(cred_f.at[p], ydev, g, 2)

    def far_reduce(g):
        @pl.when(jnp.logical_and(live(g), far))
        def _():
            slot = lax.rem(g, 2)
            f_send(g, 0).wait_recv()
            w_copy(0, g, 0).wait()

            @pl.when(g >= 2)
            def _():
                round_send(g - 2).wait_send()
            bst[slot] = new_rows(g, 0, part0[slot], recv0[slot])
            need(cred_round, g, 4)
            round_send(g).start()
            credit(cred_f.at[0], ydev, g, 2)

    def round_relay(g):
        @pl.when(jnp.logical_and(live(g - 1), home))
        def _():
            round_pass(g - 1).wait_send()
            credit(cred_round, xdev, g - 1, 4)

        @pl.when(jnp.logical_and(live(g), home))
        def _():
            round_send(g).wait_recv()
            round_pass(g).start()

    def round_take(g):
        sent(g - 1, 0, far, True)

        @pl.when(jnp.logical_and(live(g), far))
        def _():
            round_pass(g).wait_recv()
            share(g, 0)

    def cross_relay(g):
        @pl.when(jnp.logical_and(live(g - 1), home))
        def _():
            cross_send(g - 1).wait_send()
            credit(cred_side, xdev, g - 1, 3)

        @pl.when(jnp.logical_and(live(g), home))
        def _():
            side_send(g).wait_recv()
            need(cred_cross, g, 2)
            cross_send(g).start()

    def cross_reduce(g):
        sent(g - 1, 2, far, True)

        @pl.when(jnp.logical_and(live(g), far))
        def _():
            side_send(g).wait_recv()
            cross_send(g).wait_recv()
            w_copy(1, g, 2).wait()
            put_rows(g, 2, new_rows(g, 2, side_in[lax.rem(g, 3)], cross_in[lax.rem(g, 2)]))
            share(g, 2)
            credit(cred_side, xdev, g, 3)
            credit(cred_cross, ydev, g, 2)

    role = jnp.where(home, 0, 1)

    def final_place(g, p):
        n = chunk_of(g, p)
        side = lax.div(n, PIECE_CHUNKS)
        f = lax.div(g, GROUPS) - FIRST_FINAL
        at = lax.rem(g, GROUPS) * span + start[p] - side * piece
        return f, lax.rem(n, PIECE_CHUNKS), pl.ds(pl.multiple_of(at, unit), size[p]), (row // 2, lax.rem(2 * row, 4) + side)

    def final_send(g, p):
        f, m, rows, owner = final_place(g, p)
        slot = lax.rem(g, 2)
        return rcopy(parts[p].at[slot], fin_ref.at[f, role, rows], fs.at[p, slot], fin_r.at[f, role, m], owner)

    def final_local(g, p):
        owner = final_place(g, p)[3]
        return jnp.logical_and(owner[0] == col, owner[1] == row)

    def final_keep(g, p):
        f, m, rows, owner = final_place(g, p)
        slot = lax.rem(g, 2)
        return pltpu.make_async_copy(parts[p].at[slot], fin_ref.at[f, 0, rows], fs.at[p, slot])

    def final_wait(g, p):
        @pl.when(final_local(g, p))
        def _():
            final_keep(g, p).wait()

        @pl.when(jnp.logical_not(final_local(g, p)))
        def _():
            final_send(g, p).wait_send()

    own_tile = 2 * col + row // 2 == row

    def substep(g, p):
        q, gq = lax.div(g, GROUPS), lax.rem(g, GROUPS)
        n = gq * 4 + p
        b, h, slot = lax.rem(q, 3), lax.rem(q, 2), lax.rem(g, 2)
        rows = size[p]
        is_live = g < LIVE_GROUPS
        side = lax.div(n, PIECE_CHUNKS)
        own_tele = jnp.logical_and(own_tile, core == side)
        take_tele = jnp.logical_and(home, is_live)

        def tele_own():
            at = gq * span + start[p] - side * piece
            return pltpu.make_async_copy(v_ref.at[pl.ds(pl.multiple_of(at, unit), rows), half_cols(h)],
                                         vbuf.at[pl.ds(0, rows)], v_sem)

        def tele_got():
            return pltpu.make_async_copy(vt_ref.at[h, tile_rows(gq, p), :], vbuf.at[pl.ds(0, rows)], v_sem)

        @pl.when(jnp.logical_and(take_tele, own_tele))
        def _():
            tele_own().start()

        @pl.when(jnp.logical_and(take_tele, jnp.logical_not(own_tele)))
        def _():
            @pl.when(q < HALVES)
            def _():
                got = vt_ref.at[h, tile_rows(gq, p), :]
                rcopy(got, got, vs.at[0, 0], vr.at[h, n], cdev).wait_recv()
            tele_got().start()

        if p in (1, 3):
            @pl.when(jnp.logical_and(live(g - 1), home))
            def _():
                w_copy(0, g - 1, p).start()
        if p == 0:
            @pl.when(jnp.logical_and(live(g - 1), far))
            def _():
                w_copy(0, g - 1, 0).start()
        if p == 1:
            @pl.when(jnp.logical_and(live(g - 2), far))
            def _():
                w_copy(1, g - 2, 2).start()

        a_copy(gq, p).wait()
        acc[0:rows] = jnp.dot(abuf[p % 2, 0:rows], xs[b], preferred_element_type=jnp.float32)
        later_gq = lax.rem(gq + 1, GROUPS) if p >= 2 else gq

        @pl.when(g < TOTAL_GROUPS - 1 if p >= 2 else jnp.bool_(True))
        def _():
            a_copy(later_gq, (p + 2) % 4).start()

        if p == 3:
            @pl.when(jnp.logical_and(gq == GROUPS - 1, q < FIRST_FINAL - 1))
            def _():
                signal(cred_c, cdev)

                @pl.when(far)
                def _():
                    signal(cred_x, xdev)
                    signal(cred_y, ydev)

        sender = {0: home, 1: far, 2: jnp.bool_(True), 3: far}[p]

        @pl.when(jnp.logical_and(live(g - 2), sender))
        def _():
            (side_send(g - 2) if p == 2 else f_send(g - 2, p)).wait_send()

        @pl.when(g - 2 >= LIVE_GROUPS)
        def _():
            final_wait(g - 2, p)

        @pl.when(is_live)
        def _():
            @pl.when(home)
            def _():
                @pl.when(own_tele)
                def _():
                    tele_own().wait()

                @pl.when(jnp.logical_not(own_tele))
                def _():
                    tele_got().wait()
                parts[p][slot] = DAMPING * acc[0:rows] + cvec[h] * vbuf[0:rows]

            @pl.when(far)
            def _():
                parts[p][slot] = DAMPING * acc[0:rows]

            if p == 2:
                need(cred_side, g, 3)
                side_send(g).start()
            else:
                @pl.when(sender)
                def _():
                    need(cred_f.at[p], g, 2)
                    f_send(g, p).start()

        @pl.when(jnp.logical_not(is_live))
        def _():
            parts[p][slot] = DAMPING * acc[0:rows]

            @pl.when(final_local(g, p))
            def _():
                final_keep(g, p).start()

            @pl.when(jnp.logical_not(final_local(g, p)))
            def _():
                final_send(g, p).start()

        if p == 0:
            take_side(g - 3, 2, home)
            take_side(g - 2, 1, far)
            far_reduce(g - 1)
        if p == 1:
            take_side(g - 3, 0, home)
            cross_reduce(g - 2)
            home_reduce(g - 1, 1)
        if p == 2:
            round_take(g - 2)
            take_side(g - 2, 3, far)
            cross_relay(g - 1)
        if p == 3:
            round_relay(g - 1)
            home_reduce(g - 1, 3)

    def group(g, carry):
        q, gq = lax.div(g, GROUPS), lax.rem(g, GROUPS)

        @pl.when(gq == 0)
        def _():
            @pl.when(q == 0)
            def _():
                gather_finish(0)

            @pl.when(q == 1)
            def _():
                gather_finish(1)

            @pl.when(q >= HALVES)
            def _():
                other = xs.at[lax.rem(q, 3), pl.ds(pl.multiple_of(n_rows - own_base, n_rows), n_rows), :]
                rcopy(other, other, csend.at[0], crecv.at[lax.rem(q, 3)], cdev).wait_recv()

            slot = lax.rem(q + 2, 4)
            others = mrecv.at[slot, pl.ds(0, 7)]
            whole = rcopy(others, others, ms.at[slot], mr.at[slot], cdev)
            whole.wait_recv()
            whole.wait_send()
            mass = jnp.sum(jnp.sum(mrecv[slot], axis=0), axis=0, keepdims=True) / verts
            cvec[lax.rem(q, 2)] = DAMPING * mass + (1.0 - DAMPING)

            @pl.when(q < FIRST_FINAL)
            def _():
                mrecv[lax.rem(q, 4), me] = jnp.zeros((8, width), jnp.float32)

        @pl.when(jnp.logical_and(gq == 1, jnp.logical_and(q >= 1, q < FIRST_FINAL)))
        def _():
            pl.semaphore_wait(cred_c, 1)

            @pl.when(home)
            def _():
                pl.semaphore_wait(cred_x, 1)
                pl.semaphore_wait(cred_y, 1)

        @pl.when(jnp.logical_and(gq == 2, jnp.logical_and(q >= 1, q - 1 < FIRST_FINAL)))
        def _():
            for k in range(1, 8):
                mass_copy(lax.rem(q - 1, 4), k).start()

        for p in range(4):
            substep(g, p)
        return carry

    lax.fori_loop(0, TOTAL_GROUPS, group, 0)

    for g in (TOTAL_GROUPS - 2, TOTAL_GROUPS - 1):
        for p in range(4):
            final_wait(jnp.int32(g), p)

    for f in range(HALVES):
        for r in range(2):
            skip = jnp.logical_and(own_tile, home) if r == 0 else jnp.bool_(False)

            @pl.when(jnp.logical_not(skip))
            def _():
                for m in range(PIECE_CHUNKS):
                    got = fin_ref.at[f, r, pl.ds(piece_start(m), size[m % 2])]
                    rcopy(got, got, fs.at[0, 0], fin_r.at[f, r, m], cdev).wait_recv()

    @pl.when(far)
    def _():
        for g in (LIVE_GROUPS - 2, LIVE_GROUPS - 1):
            round_send(jnp.int32(g)).wait_send()

    @pl.when(jnp.logical_not(keeps))
    def _():
        for h in range(HALVES):
            for m in range(PIECE_CHUNKS):
                tele_send(h, m).wait_send()


def dang_kernel(d_ref, all_ref, send_sem, recv_sem):
    me = lax.axis_index("col") * 4 + lax.axis_index("row")
    barrier = pltpu.get_barrier_semaphore()
    others = [lax.rem(me + k, 8) for k in range(1, 8)]
    for d in others:
        signal(barrier, (d // 4, lax.rem(d, 4)))
    pl.semaphore_wait(barrier, 7)
    for d in others:
        rcopy(d_ref, all_ref.at[me], send_sem, recv_sem, (d // 4, lax.rem(d, 4))).start()
    all_ref[me] = d_ref[...]
    seven = all_ref.at[pl.ds(0, 7)]
    whole = rcopy(seven, seven, send_sem, recv_sem, (0, 0))
    whole.wait_recv()
    whole.wait_send()


def solution(mesh):
    def step(mat, x_piece, v_piece, dang_piece):
        i = lax.axis_index('row')
        n_rows, n_cols = mat.shape
        piece, vecs = x_piece.shape
        width = vecs // HALVES
        unit = n_rows // 96
        small, large = UNITS[0] * unit, UNITS[1] * unit
        lanes = min(128, width)

        dang_f = dang_piece.astype(jnp.float32)
        dang_all = pl.pallas_call(
            dang_kernel,
            out_shape=jax.ShapeDtypeStruct((8, piece // 128, 128), jnp.float32),
            in_specs=[pl.BlockSpec(memory_space=pltpu.VMEM)],
            out_specs=pl.BlockSpec(memory_space=pltpu.VMEM),
            scratch_shapes=[pltpu.SemaphoreType.DMA, pltpu.SemaphoreType.DMA],
            compiler_params=pltpu.CompilerParams(collective_id=1, has_side_effects=True),
        )(dang_f.reshape(piece // 128, 128)).reshape(-1)
        tiles = jnp.stack([lax.dynamic_slice(dang_all, (i * n_rows,), (n_rows,)),
                           lax.dynamic_slice(dang_all, (lax.rem(i + 2, 4) * n_rows,), (n_rows,))])
        weight = jnp.broadcast_to(tiles[:, :, None], (2, n_rows, lanes))
        x0 = jnp.stack([x_piece[:, h * width:(h + 1) * width] for h in range(HALVES)]).astype(jnp.bfloat16)
        m0 = jnp.sum((dang_f[:, None] * x_piece).reshape(piece // 8, 8, vecs), axis=0)
        m0 = jnp.stack([m0[:, h * width:(h + 1) * width] for h in range(HALVES)])

        f32, bf16 = jnp.float32, jnp.bfloat16
        dma, regular = pltpu.SemaphoreType.DMA, pltpu.SemaphoreType.REGULAR
        hbm = pl.BlockSpec(memory_space=pl.ANY)
        fin, _, scale = pl.pallas_call(
            kernel,
            out_shape=[jax.ShapeDtypeStruct((HALVES, 2, piece, width), f32),
                       jax.ShapeDtypeStruct((HALVES, n_rows, width), f32),
                       jax.ShapeDtypeStruct((HALVES, 1, width), f32)],
            in_specs=[hbm, hbm, hbm, hbm, pl.BlockSpec(memory_space=pltpu.VMEM)],
            out_specs=[hbm, hbm, pl.BlockSpec(memory_space=pltpu.VMEM)],
            scratch_shapes=[
                pltpu.VMEM((3, n_cols, width), bf16),
                pltpu.VMEM((2, large, n_cols), bf16),
                pltpu.VMEM((large, width), f32),
                pltpu.VMEM((2, small, width), f32),
                pltpu.VMEM((2, large, width), f32),
                pltpu.VMEM((2, small, width), f32),
                pltpu.VMEM((2, large, width), f32),
                pltpu.VMEM((2, small, width), f32),
                pltpu.VMEM((2, large, width), f32),
                pltpu.VMEM((2, large, width), f32),
                pltpu.VMEM((3, small, width), f32),
                pltpu.VMEM((2, small, width), f32),
                pltpu.VMEM((2, small, width), bf16),
                pltpu.VMEM((4, small, width), bf16),
                pltpu.VMEM((large, width), f32),
                pltpu.VMEM((large, lanes), f32),
                pltpu.VMEM((4, 8, 8, width), f32),
                dma((2,)), dma, dma,
                dma((4, 2)), dma((4, 2)),
                dma((3,)), dma, dma((2,)),
                dma((2,)), dma((4,)), dma, dma((2, GROUPS)),
                dma((4,)), dma((2, CHUNKS)), dma((4,)), dma((3,)),
                dma((2,)), dma((2,)), dma((2,)), dma((2,)), dma((2,)), dma((2,)), dma((2,)),
                dma((2, PIECE_CHUNKS)), dma((2, CHUNKS)),
                dma((4,)), dma((4,)), dma((2, 2, PIECE_CHUNKS)),
                regular((4,)), regular, regular, regular, regular, regular, regular,
            ],
            compiler_params=pltpu.CompilerParams(collective_id=0, has_side_effects=True,
                                                 vmem_limit_bytes=62 * 1024 * 1024),
            cost_estimate=pl.CostEstimate(flops=2 * n_rows * n_cols * vecs * SWEEPS,
                                          bytes_accessed=n_rows * n_cols * 2 * PHASES, transcendentals=0),
        )(mat, x0, v_piece, weight, m0)
        halves = [(fin[h, 0] + fin[h, 1]) + scale[h] * v_piece[:, h * width:(h + 1) * width] for h in range(HALVES)]
        return jnp.concatenate(halves, axis=1)

    vec = P(('col', 'row'), None)
    return jax.shard_map(step, mesh=mesh, in_specs=(P('row', 'col'), vec, vec, P(('col', 'row'))),
                         out_specs=vec, check_vma=False)
```

```python
import jax
import jax.numpy as jnp
from jax import lax
from jax.experimental import pallas as pl
from jax.experimental.pallas import tpu as pltpu
from jax.sharding import PartitionSpec as P

SWEEPS = 8
DAMPING = 0.85
MESH = pl.DeviceIdType.MESH
HALVES = 2
PHASES = SWEEPS * HALVES
GROUPS = 3
CHUNKS = 4 * GROUPS
PIECE_CHUNKS = CHUNKS // 2
KSTEPS = 3
UNITS = (7, 9, 7, 9)
FIRST_FINAL = PHASES - HALVES
LIVE_GROUPS = FIRST_FINAL * GROUPS
TOTAL_GROUPS = PHASES * GROUPS


def rcopy(src, dst, send_sem, recv_sem, dev):
    return pltpu.make_async_remote_copy(src_ref=src, dst_ref=dst, send_sem=send_sem, recv_sem=recv_sem,
                                        device_id={"col": dev[0], "row": dev[1]}, device_id_type=MESH)


def signal(sem, dev):
    pl.semaphore_signal(sem, inc=1, device_id={"col": dev[0], "row": dev[1]}, device_id_type=MESH)


def kernel(a_ref, x0_ref, v_ref, w_ref, m0_ref, fin_ref, vt_ref, cvec,
           xs, abuf, acc, part0, part1, part2, part3, recv0, recv1, recv3, side_in, cross_in, bst, round_in,
           vbuf, wbuf, mrecv,
           a_sem, v_sem, w_sem,
           fs, fr, side_r, cross_s, cross_r, bs, round_r, round_s, yrecv, xsend, xrecv, csend, crecv,
           gx_s, gx_r, gc_s, gc_r, gl_s, gl_r, g_loc, vs, vr,
           ms, mr, fin_r, cred_f, cred_side, cred_cross, cred_round, cred_c, cred_x, cred_y):
    col, row = lax.axis_index("col"), lax.axis_index("row")
    core = lax.rem(row, 2)
    home = col == row // 2
    far = jnp.logical_not(home)
    ydev = (1 - col, row)
    xdev = (col, lax.rem(row + 2, 4))
    cdev = (col, row + 1 - 2 * core)
    me = col * 4 + row
    n_rows, n_cols = a_ref.shape
    verts = n_cols * 2
    unit = n_rows // 96
    size = tuple(u * unit for u in UNITS)
    start = (0, size[0], size[0] + size[1], size[0] + size[1] + size[2])
    span = sum(size)
    piece = n_rows // 2
    width = x0_ref.shape[2]
    own_base = core * n_rows
    parts = (part0, part1, part2, part3)
    recvs = (recv0, recv1, None, recv3)

    def every_other(k):
        d = lax.rem(me + k, 8)
        return (d // 4, lax.rem(d, 4))

    def tile_rows(gq, p):
        return pl.ds(pl.multiple_of(gq * span + start[p], unit), size[p])

    def half_cols(h):
        return pl.ds(pl.multiple_of(h * width, width), width)

    depth = n_cols // KSTEPS

    def a_copy(gq, p, kb):
        return pltpu.make_async_copy(
            a_ref.at[tile_rows(gq, p), pl.ds(pl.multiple_of(kb * depth, depth), depth)],
            abuf.at[p % 2, kb, pl.ds(0, size[p])], a_sem.at[p % 2, kb])

    for p in range(2):
        for kb in range(KSTEPS):
            a_copy(0, p, kb).start()

    barrier = pltpu.get_barrier_semaphore()
    for k in range(1, 8):
        signal(barrier, every_other(k))
    pl.semaphore_wait(barrier, 7)

    def x_rows(h, r):
        return xs.at[h, pl.ds(pl.multiple_of(r * piece, piece), piece), :]

    def gather_own(h):
        return pltpu.make_async_copy(x0_ref.at[h], x_rows(h, row), g_loc.at[h])

    def gather_x(h):
        return rcopy(x0_ref.at[h], x_rows(h, row), gx_s.at[h], gx_r.at[h], xdev)

    def gather_c(h):
        return rcopy(x0_ref.at[h], x_rows(h, row), gc_s.at[h], gc_r.at[h], cdev)

    def gather_relay(h):
        r = lax.rem(row + 2, 4)
        return rcopy(x_rows(h, r), x_rows(h, r), gl_s.at[h], gl_r.at[h], cdev)

    keeper = (col, 2 * col + row // 2)
    keeps = jnp.logical_and(home, row == keeper[1])

    def piece_start(m):
        return (m // 2) * (size[0] + size[1]) + (m % 2) * size[0]

    def tele_send(h, m):
        rows = size[m % 2]
        src = v_ref.at[pl.ds(piece_start(m), rows), pl.ds(h * width, width)]
        dst = vt_ref.at[h, pl.ds(pl.multiple_of(core * piece + piece_start(m), unit), rows), :]
        return rcopy(src, dst, vs.at[h, m], vr.at[h, core * PIECE_CHUNKS + m], keeper)

    def mass_copy(slot, k):
        return rcopy(mrecv.at[slot, me], mrecv.at[slot, me], ms.at[slot], mr.at[slot], every_other(k))

    for h in range(HALVES):
        mrecv[2 + h, me] = m0_ref[h]
        for k in range(1, 8):
            mass_copy(2 + h, k).start()

    for h in range(HALVES):
        gather_x(h).start()
        gather_c(h).start()
        gather_own(h).start()

        @pl.when(jnp.logical_not(keeps))
        def _():
            for m in range(PIECE_CHUNKS):
                tele_send(h, m).start()

    def gather_finish(h):
        gather_x(h).wait_recv()
        gather_relay(h).start()
        gather_own(h).wait()
        gather_c(h).wait_recv()
        gather_relay(h).wait_recv()
        gather_x(h).wait_send()
        gather_c(h).wait_send()
        gather_relay(h).wait_send()

    def live(g):
        return jnp.logical_and(g >= 0, g < LIVE_GROUPS)

    def own_rows(g, p):
        b = lax.rem(lax.div(g, GROUPS) + 2, 3)
        gq = lax.rem(g, GROUPS)
        return xs.at[b, pl.ds(pl.multiple_of(own_base + gq * span + start[p], unit), size[p]), :]

    def chunk_of(g, p):
        return lax.rem(g, GROUPS) * 4 + p

    def parity(g):
        return lax.rem(lax.div(g, GROUPS), 2)

    def f_send(g, p):
        slot = lax.rem(g, 2)
        return rcopy(parts[p].at[slot], recvs[p].at[slot], fs.at[p, slot], fr.at[p, slot], ydev)

    def side_send(g):
        slot, in_slot = lax.rem(g, 2), lax.rem(g, 3)
        return rcopy(part2.at[slot], side_in.at[in_slot], fs.at[2, slot], side_r.at[in_slot], xdev)

    def cross_send(g):
        slot, in_slot = lax.rem(g, 2), lax.rem(g, 3)
        return rcopy(side_in.at[in_slot], cross_in.at[slot], cross_s, cross_r.at[slot], ydev)

    def round_send(g):
        slot, in_slot = lax.rem(g, 2), lax.rem(g, 4)
        return rcopy(bst.at[slot], round_in.at[in_slot], bs.at[slot], round_r.at[in_slot], xdev)

    def round_pass(g):
        in_slot = lax.rem(g, 4)
        return rcopy(round_in.at[in_slot], own_rows(g, 0), round_s, yrecv.at[parity(g), lax.rem(g, GROUPS)], ydev)

    def x_send(g, p):
        return rcopy(own_rows(g, p), own_rows(g, p), xsend.at[p], xrecv.at[parity(g), chunk_of(g, p)], xdev)

    def c_send(g, p):
        b = lax.rem(lax.div(g, GROUPS) + 2, 3)
        return rcopy(own_rows(g, p), own_rows(g, p), csend.at[p], crecv.at[b], cdev)

    def w_copy(which, g, p):
        return pltpu.make_async_copy(w_ref.at[which, tile_rows(lax.rem(g, GROUPS), p), :],
                                     wbuf.at[pl.ds(0, size[p])], w_sem)

    def new_rows(g, p, one, two):
        x = one + two
        w = wbuf[0:size[p]]
        lanes = w.shape[1]
        wx = jnp.concatenate([x[:, k * lanes:(k + 1) * lanes] * w for k in range(width // lanes)], axis=1)
        slot = lax.rem(lax.div(g, GROUPS), 4)
        mrecv[slot, me] = mrecv[slot, me] + jnp.sum(wx.reshape(size[p] // 8, 8, width), axis=0)
        return x.astype(jnp.bfloat16)

    def put_rows(g, p, value):
        b = lax.rem(lax.div(g, GROUPS) + 2, 3)
        gq = lax.rem(g, GROUPS)
        xs[b, pl.ds(pl.multiple_of(own_base + gq * span + start[p], unit), size[p]), :] = value

    def share(g, p):
        x_send(g, p).start()
        c_send(g, p).start()

    def sent(g, p, role, both):
        @pl.when(jnp.logical_and(live(g), role))
        def _():
            if both:
                x_send(g, p).wait_send()
            c_send(g, p).wait_send()

    def take_side(g, p, role):
        sent(g - 1, p, role, False)

        @pl.when(jnp.logical_and(live(g), role))
        def _():
            x_send(g, p).wait_recv()
            c_send(g, p).start()

    def credit(sem, dev, g, depth_):
        @pl.when(g < LIVE_GROUPS - depth_)
        def _():
            signal(sem, dev)

    def need(sem, g, depth_):
        @pl.when(g >= depth_)
        def _():
            pl.semaphore_wait(sem, 1)

    def home_reduce(g, p):
        sent(g - 1, p, home, True)

        @pl.when(jnp.logical_and(live(g), home))
        def _():
            slot = lax.rem(g, 2)
            f_send(g, p).wait_recv()
            w_copy(0, g, p).wait()
            put_rows(g, p, new_rows(g, p, parts[p][slot], recvs[p][slot]))
            share(g, p)
            credit(cred_f.at[p], ydev, g, 2)

    def far_reduce(g):
        @pl.when(jnp.logical_and(live(g), far))
        def _():
            slot = lax.rem(g, 2)
            f_send(g, 0).wait_recv()
            w_copy(0, g, 0).wait()

            @pl.when(g >= 2)
            def _():
                round_send(g - 2).wait_send()
            bst[slot] = new_rows(g, 0, part0[slot], recv0[slot])
            need(cred_round, g, 4)
            round_send(g).start()
            credit(cred_f.at[0], ydev, g, 2)

    def round_relay(g):
        @pl.when(jnp.logical_and(live(g - 1), home))
        def _():
            round_pass(g - 1).wait_send()
            credit(cred_round, xdev, g - 1, 4)

        @pl.when(jnp.logical_and(live(g), home))
        def _():
            round_send(g).wait_recv()
            round_pass(g).start()

    def round_take(g):
        sent(g - 1, 0, far, True)

        @pl.when(jnp.logical_and(live(g), far))
        def _():
            round_pass(g).wait_recv()
            share(g, 0)

    def cross_relay(g):
        @pl.when(jnp.logical_and(live(g - 1), home))
        def _():
            cross_send(g - 1).wait_send()
            credit(cred_side, xdev, g - 1, 3)

        @pl.when(jnp.logical_and(live(g), home))
        def _():
            side_send(g).wait_recv()
            need(cred_cross, g, 2)
            cross_send(g).start()

    def cross_reduce(g):
        sent(g - 1, 2, far, True)

        @pl.when(jnp.logical_and(live(g), far))
        def _():
            side_send(g).wait_recv()
            cross_send(g).wait_recv()
            w_copy(1, g, 2).wait()
            put_rows(g, 2, new_rows(g, 2, side_in[lax.rem(g, 3)], cross_in[lax.rem(g, 2)]))
            share(g, 2)
            credit(cred_side, xdev, g, 3)
            credit(cred_cross, ydev, g, 2)

    role = jnp.where(home, 0, 1)

    def final_place(g, p):
        n = chunk_of(g, p)
        side = lax.div(n, PIECE_CHUNKS)
        f = lax.div(g, GROUPS) - FIRST_FINAL
        at = lax.rem(g, GROUPS) * span + start[p] - side * piece
        return f, lax.rem(n, PIECE_CHUNKS), pl.ds(pl.multiple_of(at, unit), size[p]), (row // 2, lax.rem(2 * row, 4) + side)

    def final_send(g, p):
        f, m, rows, owner = final_place(g, p)
        slot = lax.rem(g, 2)
        return rcopy(parts[p].at[slot], fin_ref.at[f, role, rows], fs.at[p, slot], fin_r.at[f, role, m], owner)

    def final_local(g, p):
        owner = final_place(g, p)[3]
        return jnp.logical_and(owner[0] == col, owner[1] == row)

    def final_keep(g, p):
        f, m, rows, owner = final_place(g, p)
        slot = lax.rem(g, 2)
        return pltpu.make_async_copy(parts[p].at[slot], fin_ref.at[f, 0, rows], fs.at[p, slot])

    def final_wait(g, p):
        @pl.when(final_local(g, p))
        def _():
            final_keep(g, p).wait()

        @pl.when(jnp.logical_not(final_local(g, p)))
        def _():
            final_send(g, p).wait_send()

    own_tile = 2 * col + row // 2 == row

    def substep(g, p):
        q, gq = lax.div(g, GROUPS), lax.rem(g, GROUPS)
        n = gq * 4 + p
        b, h, slot = lax.rem(q, 3), lax.rem(q, 2), lax.rem(g, 2)
        rows = size[p]
        is_live = g < LIVE_GROUPS
        side = lax.div(n, PIECE_CHUNKS)
        own_tele = jnp.logical_and(own_tile, core == side)
        take_tele = jnp.logical_and(home, is_live)

        def tele_own():
            at = gq * span + start[p] - side * piece
            return pltpu.make_async_copy(v_ref.at[pl.ds(pl.multiple_of(at, unit), rows), half_cols(h)],
                                         vbuf.at[pl.ds(0, rows)], v_sem)

        def tele_got():
            return pltpu.make_async_copy(vt_ref.at[h, tile_rows(gq, p), :], vbuf.at[pl.ds(0, rows)], v_sem)

        @pl.when(jnp.logical_and(take_tele, own_tele))
        def _():
            tele_own().start()

        @pl.when(jnp.logical_and(take_tele, jnp.logical_not(own_tele)))
        def _():
            @pl.when(q < HALVES)
            def _():
                got = vt_ref.at[h, tile_rows(gq, p), :]
                rcopy(got, got, vs.at[0, 0], vr.at[h, n], cdev).wait_recv()
            tele_got().start()

        if p in (1, 3):
            @pl.when(jnp.logical_and(live(g - 1), home))
            def _():
                w_copy(0, g - 1, p).start()
        if p == 0:
            @pl.when(jnp.logical_and(live(g - 1), far))
            def _():
                w_copy(0, g - 1, 0).start()
        if p == 1:
            @pl.when(jnp.logical_and(live(g - 2), far))
            def _():
                w_copy(1, g - 2, 2).start()

        later_gq = lax.rem(gq + 1, GROUPS) if p >= 2 else gq
        more = g < TOTAL_GROUPS - 1 if p >= 2 else jnp.bool_(True)
        acc[0:rows] = jnp.zeros((rows, width), jnp.float32)

        def kstep(kb, carry):
            a_copy(gq, p, kb).wait()
            acc[0:rows] += jnp.dot(abuf[p % 2, kb, 0:rows], xs[b, pl.ds(pl.multiple_of(kb * depth, depth), depth), :],
                                   preferred_element_type=jnp.float32)

            @pl.when(more)
            def _():
                a_copy(later_gq, (p + 2) % 4, kb).start()
            return carry

        lax.fori_loop(0, KSTEPS, kstep, 0)

        if p == 3:
            @pl.when(jnp.logical_and(gq == GROUPS - 1, q < FIRST_FINAL - 1))
            def _():
                signal(cred_c, cdev)

                @pl.when(far)
                def _():
                    signal(cred_x, xdev)
                    signal(cred_y, ydev)

        sender = {0: home, 1: far, 2: jnp.bool_(True), 3: far}[p]

        @pl.when(jnp.logical_and(live(g - 2), sender))
        def _():
            (side_send(g - 2) if p == 2 else f_send(g - 2, p)).wait_send()

        @pl.when(g - 2 >= LIVE_GROUPS)
        def _():
            final_wait(g - 2, p)

        @pl.when(is_live)
        def _():
            @pl.when(home)
            def _():
                @pl.when(own_tele)
                def _():
                    tele_own().wait()

                @pl.when(jnp.logical_not(own_tele))
                def _():
                    tele_got().wait()
                parts[p][slot] = DAMPING * acc[0:rows] + cvec[h] * vbuf[0:rows]

            @pl.when(far)
            def _():
                parts[p][slot] = DAMPING * acc[0:rows]

            if p == 2:
                need(cred_side, g, 3)
                side_send(g).start()
            else:
                @pl.when(sender)
                def _():
                    need(cred_f.at[p], g, 2)
                    f_send(g, p).start()

        @pl.when(jnp.logical_not(is_live))
        def _():
            parts[p][slot] = DAMPING * acc[0:rows]

            @pl.when(final_local(g, p))
            def _():
                final_keep(g, p).start()

            @pl.when(jnp.logical_not(final_local(g, p)))
            def _():
                final_send(g, p).start()

        if p == 0:
            take_side(g - 3, 2, home)
            take_side(g - 2, 1, far)
            far_reduce(g - 1)
        if p == 1:
            take_side(g - 3, 0, home)
            cross_reduce(g - 2)
            home_reduce(g - 1, 1)
        if p == 2:
            round_take(g - 2)
            take_side(g - 2, 3, far)
            cross_relay(g - 1)
        if p == 3:
            round_relay(g - 1)
            home_reduce(g - 1, 3)

    def group(g, carry):
        q, gq = lax.div(g, GROUPS), lax.rem(g, GROUPS)

        @pl.when(gq == 0)
        def _():
            @pl.when(q == 0)
            def _():
                gather_finish(0)

            @pl.when(q == 1)
            def _():
                gather_finish(1)

            @pl.when(q >= HALVES)
            def _():
                other = xs.at[lax.rem(q, 3), pl.ds(pl.multiple_of(n_rows - own_base, n_rows), n_rows), :]
                rcopy(other, other, csend.at[0], crecv.at[lax.rem(q, 3)], cdev).wait_recv()

            slot = lax.rem(q + 2, 4)
            others = mrecv.at[slot, pl.ds(0, 7)]
            whole = rcopy(others, others, ms.at[slot], mr.at[slot], cdev)
            whole.wait_recv()
            whole.wait_send()
            mass = jnp.sum(jnp.sum(mrecv[slot], axis=0), axis=0, keepdims=True) / verts
            cvec[lax.rem(q, 2)] = DAMPING * mass + (1.0 - DAMPING)

            @pl.when(q < FIRST_FINAL)
            def _():
                mrecv[lax.rem(q, 4), me] = jnp.zeros((8, width), jnp.float32)

        @pl.when(jnp.logical_and(gq == 1, jnp.logical_and(q >= 1, q < FIRST_FINAL)))
        def _():
            pl.semaphore_wait(cred_c, 1)

            @pl.when(home)
            def _():
                pl.semaphore_wait(cred_x, 1)
                pl.semaphore_wait(cred_y, 1)

        @pl.when(jnp.logical_and(gq == 2, jnp.logical_and(q >= 1, q - 1 < FIRST_FINAL)))
        def _():
            for k in range(1, 8):
                mass_copy(lax.rem(q - 1, 4), k).start()

        for p in range(4):
            substep(g, p)
        return carry

    lax.fori_loop(0, TOTAL_GROUPS, group, 0)

    for g in (TOTAL_GROUPS - 2, TOTAL_GROUPS - 1):
        for p in range(4):
            final_wait(jnp.int32(g), p)

    for f in range(HALVES):
        for r in range(2):
            skip = jnp.logical_and(own_tile, home) if r == 0 else jnp.bool_(False)

            @pl.when(jnp.logical_not(skip))
            def _():
                for m in range(PIECE_CHUNKS):
                    got = fin_ref.at[f, r, pl.ds(piece_start(m), size[m % 2])]
                    rcopy(got, got, fs.at[0, 0], fin_r.at[f, r, m], cdev).wait_recv()

    @pl.when(far)
    def _():
        for g in (LIVE_GROUPS - 2, LIVE_GROUPS - 1):
            round_send(jnp.int32(g)).wait_send()

    @pl.when(jnp.logical_not(keeps))
    def _():
        for h in range(HALVES):
            for m in range(PIECE_CHUNKS):
                tele_send(h, m).wait_send()


def dang_kernel(d_ref, all_ref, send_sem, recv_sem):
    me = lax.axis_index("col") * 4 + lax.axis_index("row")
    barrier = pltpu.get_barrier_semaphore()
    others = [lax.rem(me + k, 8) for k in range(1, 8)]
    for d in others:
        signal(barrier, (d // 4, lax.rem(d, 4)))
    pl.semaphore_wait(barrier, 7)
    for d in others:
        rcopy(d_ref, all_ref.at[me], send_sem, recv_sem, (d // 4, lax.rem(d, 4))).start()
    all_ref[me] = d_ref[...]
    seven = all_ref.at[pl.ds(0, 7)]
    whole = rcopy(seven, seven, send_sem, recv_sem, (0, 0))
    whole.wait_recv()
    whole.wait_send()


def solution(mesh):
    def step(mat, x_piece, v_piece, dang_piece):
        i = lax.axis_index('row')
        n_rows, n_cols = mat.shape
        piece, vecs = x_piece.shape
        width = vecs // HALVES
        unit = n_rows // 96
        small, large = UNITS[0] * unit, UNITS[1] * unit
        lanes = min(128, width)

        dang_f = dang_piece.astype(jnp.float32)
        dang_all = pl.pallas_call(
            dang_kernel,
            out_shape=jax.ShapeDtypeStruct((8, piece // 128, 128), jnp.float32),
            in_specs=[pl.BlockSpec(memory_space=pltpu.VMEM)],
            out_specs=pl.BlockSpec(memory_space=pltpu.VMEM),
            scratch_shapes=[pltpu.SemaphoreType.DMA, pltpu.SemaphoreType.DMA],
            compiler_params=pltpu.CompilerParams(collective_id=1, has_side_effects=True),
        )(dang_f.reshape(piece // 128, 128)).reshape(-1)
        tiles = jnp.stack([lax.dynamic_slice(dang_all, (i * n_rows,), (n_rows,)),
                           lax.dynamic_slice(dang_all, (lax.rem(i + 2, 4) * n_rows,), (n_rows,))])
        weight = jnp.broadcast_to(tiles[:, :, None], (2, n_rows, lanes))
        x0 = jnp.stack([x_piece[:, h * width:(h + 1) * width] for h in range(HALVES)]).astype(jnp.bfloat16)
        m0 = jnp.sum((dang_f[:, None] * x_piece).reshape(piece // 8, 8, vecs), axis=0)
        m0 = jnp.stack([m0[:, h * width:(h + 1) * width] for h in range(HALVES)])

        f32, bf16 = jnp.float32, jnp.bfloat16
        dma, regular = pltpu.SemaphoreType.DMA, pltpu.SemaphoreType.REGULAR
        hbm = pl.BlockSpec(memory_space=pl.ANY)
        fin, _, scale = pl.pallas_call(
            kernel,
            out_shape=[jax.ShapeDtypeStruct((HALVES, 2, piece, width), f32),
                       jax.ShapeDtypeStruct((HALVES, n_rows, width), f32),
                       jax.ShapeDtypeStruct((HALVES, 1, width), f32)],
            in_specs=[hbm, hbm, hbm, hbm, pl.BlockSpec(memory_space=pltpu.VMEM)],
            out_specs=[hbm, hbm, pl.BlockSpec(memory_space=pltpu.VMEM)],
            scratch_shapes=[
                pltpu.VMEM((3, n_cols, width), bf16),
                pltpu.VMEM((2, KSTEPS, large, n_cols // KSTEPS), bf16),
                pltpu.VMEM((large, width), f32),
                pltpu.VMEM((2, small, width), f32),
                pltpu.VMEM((2, large, width), f32),
                pltpu.VMEM((2, small, width), f32),
                pltpu.VMEM((2, large, width), f32),
                pltpu.VMEM((2, small, width), f32),
                pltpu.VMEM((2, large, width), f32),
                pltpu.VMEM((2, large, width), f32),
                pltpu.VMEM((3, small, width), f32),
                pltpu.VMEM((2, small, width), f32),
                pltpu.VMEM((2, small, width), bf16),
                pltpu.VMEM((4, small, width), bf16),
                pltpu.VMEM((large, width), f32),
                pltpu.VMEM((large, lanes), f32),
                pltpu.VMEM((4, 8, 8, width), f32),
                dma((2, KSTEPS)), dma, dma,
                dma((4, 2)), dma((4, 2)),
                dma((3,)), dma, dma((2,)),
                dma((2,)), dma((4,)), dma, dma((2, GROUPS)),
                dma((4,)), dma((2, CHUNKS)), dma((4,)), dma((3,)),
                dma((2,)), dma((2,)), dma((2,)), dma((2,)), dma((2,)), dma((2,)), dma((2,)),
                dma((2, PIECE_CHUNKS)), dma((2, CHUNKS)),
                dma((4,)), dma((4,)), dma((2, 2, PIECE_CHUNKS)),
                regular((4,)), regular, regular, regular, regular, regular, regular,
            ],
            compiler_params=pltpu.CompilerParams(collective_id=0, has_side_effects=True,
                                                 vmem_limit_bytes=62 * 1024 * 1024),
            cost_estimate=pl.CostEstimate(flops=2 * n_rows * n_cols * vecs * SWEEPS,
                                          bytes_accessed=n_rows * n_cols * 2 * PHASES, transcendentals=0),
        )(mat, x0, v_piece, weight, m0)
        halves = [(fin[h, 0] + fin[h, 1]) + scale[h] * v_piece[:, h * width:(h + 1) * width] for h in range(HALVES)]
        return jnp.concatenate(halves, axis=1)

    vec = P(('col', 'row'), None)
    return jax.shard_map(step, mesh=mesh, in_specs=(P('row', 'col'), vec, vec, P(('col', 'row'))),
                         out_specs=vec, check_vma=False)
```
